1024 devices in a mesh: wide: 32 (over y, z_lo), fields: 32 (over x, z_hi, core).
Axes of the slice: x: 8, y: 8, z: 8 (z_hi: 2, z_lo: 4; z = z_hi * 4 + z_lo), core: 2. Of those that a mesh axis runs over, the one named last changes fastest.
Arguments:
- vectors: float32 [1024, 16384], P('wide', 'fields'), may hold values from 0.03 to 82, as said below
- pivot_ids: int32 [8], replicated, may hold values from 0 to 1023
Outputs:
- similarity: float32 [1024, 4, 256], P('wide', None, 'fields')
The draws below stay inside these ranges and needn't reach their ends.
Inputs may be any that keep to these rules, and one draw needn't show every extreme that they name: `vectors`: every entry is positive.
All inputs are finite; a program needn't handle non-finite values.
Results may differ from the reference program's by a relative error of at most 0.0003.
Values sent between devices are 32-bit elements; how exact they have to be, the bound alone decides.
No kernel may reach another device: no remote copies, remote signals or barrier semaphores. Data moves between devices by JAX's collectives and lax.ppermute only.
A program may use at most 32 MiB of HBM per device.

```python
import math
import jax
import jax.numpy as jnp
from jax import lax

F = 16384
VB = 32
P_SIZE = 8
STEPS = 4
NVEC = 1024
N_WIDE = 32


def draw_vectors(key, part):
    first, second, third = jax.random.split(jax.random.fold_in(key, 11), 3)
    base = jnp.exp(jax.random.uniform(first, (NVEC, F), jnp.float32, -1.0, 1.0))
    row_scale = jnp.exp(jax.random.uniform(second, (NVEC, 1), jnp.float32, 0.0, math.log(10.0)))
    column_scale = jnp.exp(jax.random.uniform(third, (1, F), jnp.float32, math.log(0.3), math.log(3.0)))
    return (base * row_scale * column_scale).astype(jnp.float32)


def set_ends(drawn, key, low, largest):
    index_at = [jax.random.randint(jax.random.fold_in(key, axis), (), 0, length) for axis, length in enumerate(drawn.shape)]
    main_axis = drawn.shape.index(max(drawn.shape))
    beside = index_at[:main_axis] + [(index_at[main_axis] + 1) % drawn.shape[main_axis]] + index_at[main_axis + 1:]
    return drawn.at[tuple(index_at)].set(low).at[tuple(beside)].set(largest)


def setup_inputs(seed: int = 0) -> dict:
    key_list = jax.random.split(jax.random.key(seed), 3)
    vectors = draw_vectors(jax.random.fold_in(key_list[2], 71), 0)
    pivot_ids = set_ends(jax.random.randint(key_list[1], (P_SIZE,), 0, NVEC), jax.random.fold_in(key_list[1], 1), 0, NVEC - 1).astype(jnp.int32)
    return dict(vectors=vectors, pivot_ids=pivot_ids)


def triple_table(owned, pivots, minima, partner):
    with_pivot = jnp.sum(minima, axis=-1)
    pivot_side = jnp.sum(jnp.minimum(pivots[:, None, :], partner[None, :, :]), axis=-1)
    pair_side = jnp.sum(jnp.minimum(owned[:, None, :], partner[None, :, :]), axis=-1)
    triple = lax.map(lambda layer: jnp.sum(jnp.minimum(layer[:, None, :], partner[None, :, :]), axis=-1), jnp.transpose(minima, (1, 0, 2)))
    return with_pivot[:, :, None] + pivot_side[None, :, :] + pair_side[:, None, :] - jnp.transpose(triple, (1, 0, 2))


def reference(vectors, pivot_ids):
    totals = jnp.sum(vectors, axis=1)
    pivots = jnp.take(vectors, pivot_ids, axis=0)
    pivot_totals = jnp.take(totals, pivot_ids, axis=0)
    blocks = vectors.reshape(N_WIDE, VB, F)
    block_totals = totals.reshape(N_WIDE, VB)

    def one_block(block_index):
        owned = blocks[block_index]
        owned_total = block_totals[block_index]
        minima = jnp.minimum(owned[:, None, :], pivots[None, :, :])
        step_rows = []
        for stride in range(1, STEPS + 1):
            source = (block_index - stride) % N_WIDE
            partner = blocks[source]
            partner_total = block_totals[source]
            numerator = triple_table(owned, pivots, minima, partner)
            denominator = owned_total[:, None, None] + pivot_totals[None, :, None] + partner_total[None, None, :]
            step_rows.append((1.5 * numerator / denominator).reshape(VB, P_SIZE * VB))
        return jnp.stack(step_rows, axis=1)

    table = lax.map(one_block, jnp.arange(N_WIDE, dtype=jnp.int32))
    return table.reshape(NVEC, STEPS, P_SIZE * VB)
```

```python
import jax
import jax.numpy as jnp
from jax import lax
from jax.experimental import pallas as pl
from jax.experimental.pallas import tpu as pltpu
from jax.sharding import PartitionSpec as P

STEPS = 4
LANES = 128
SUBLANES = 8
SHARE_ROWS = SUBLANES + 1


def from_behind(value, axis, steps):
    count = lax.axis_size(axis)
    pairs = [(source, (source + steps) % count) for source in range(count)]
    return lax.ppermute(value, axis, pairs)


def to_everyone(copies, axis):
    return lax.all_to_all(copies, axis, split_axis=0, concat_axis=0, tiled=True)


def spread_kernel(ids_ref, vectors_ref, copies_ref, rows_ref):
    row_count = vectors_ref.shape[0]
    for q in range(rows_ref.shape[0]):
        rows_ref[q : q + 1, :] = vectors_ref[pl.ds(lax.rem(ids_ref[q], row_count), 1), :]
    rows = rows_ref[...]
    for peer in range(copies_ref.shape[0]):
        copies_ref[peer] = rows


def lane_at(offset):
    lane = lax.broadcasted_iota(jnp.int32, (SUBLANES, LANES), 1)
    sublane = lax.broadcasted_iota(jnp.int32, (SUBLANES, LANES), 0)
    return lane == sublane + offset


def column_sum(tiles):
    folded = tiles[0]
    for tile in tiles[1:]:
        folded = folded + tile
    return jnp.sum(folded, axis=1, keepdims=True)


def row_of(columns):
    row = jnp.zeros((SUBLANES, LANES), jnp.float32)
    for offset, column in columns:
        row = row + jnp.where(lane_at(offset), column, 0.0)
    return jnp.sum(row, axis=0, keepdims=True)


def table_kernel(ids_ref, own_ref, arrived_ref, *refs):
    partner_refs = refs[:STEPS]
    out_ref, pivots_ref, larger_ref = refs[STEPS:]
    row_count, width = own_ref.shape
    pivot_count = pivots_ref.shape[0]
    tiles = width // LANES
    v_tiles = row_count // SUBLANES
    q_lanes = LANES // row_count
    q_tiles = pivot_count // q_lanes
    for q in range(pivot_count):
        pivots_ref[q : q + 1, :] = arrived_ref[lax.div(ids_ref[q], row_count), q : q + 1, :]

    smaller = []
    for qt in range(q_tiles):
        columns = []
        for ql in range(q_lanes):
            q = qt * q_lanes + ql
            for vt in range(v_tiles):
                low = [
                    jnp.minimum(
                        own_ref[vt * SUBLANES : (vt + 1) * SUBLANES, t * LANES : (t + 1) * LANES],
                        pivots_ref[q : q + 1, t * LANES : (t + 1) * LANES],
                    )
                    for t in range(tiles)
                ]
                columns.append((ql * row_count + vt * SUBLANES, column_sum(low)))
        smaller.append(row_of(columns))
        for t in range(tiles):
            at = slice(t * LANES, (t + 1) * LANES)
            high = jnp.concatenate(
                [
                    jnp.maximum(own_ref[:, at], pivots_ref[qt * q_lanes + ql : qt * q_lanes + ql + 1, at])
                    for ql in range(q_lanes)
                ],
                axis=0,
            )
            larger_ref[qt, at, :] = high.T

    def some_fields(t, sums):
        at = pl.ds(t * LANES, LANES)
        blocks = [
            ref[vt * SUBLANES : (vt + 1) * SUBLANES, at] for ref in partner_refs for vt in range(v_tiles)
        ]
        sums = list(sums)
        for f in range(LANES):
            rows = [
                jnp.broadcast_to(larger_ref[qt, pl.ds(t * LANES + f, 1), :], (SUBLANES, LANES))
                for qt in range(q_tiles)
            ]
            for i, block in enumerate(blocks):
                x = jnp.broadcast_to(block[:, f : f + 1], (SUBLANES, LANES))
                for qt in range(q_tiles):
                    k = i * q_tiles + qt
                    sums[k] = sums[k] + jnp.minimum(x, rows[qt])
        return tuple(sums)

    first = tuple(
        jnp.broadcast_to(smaller[k % q_tiles], (SUBLANES, LANES))
        for k in range(STEPS * v_tiles * q_tiles)
    )
    sums = lax.fori_loop(0, tiles, some_fields, first)

    for vt in range(v_tiles):
        for q in range(pivot_count):
            qt, ql = divmod(q, q_lanes)
            lanes = slice(ql * row_count, (ql + 1) * row_count)
            tile = jnp.concatenate(
                [sums[(s * v_tiles + vt) * q_tiles + qt][:, lanes] for s in range(STEPS)], axis=1
            )
            at = (q * v_tiles + vt) * SHARE_ROWS
            out_ref[at : at + SUBLANES, :] = tile

    def totals(ref, vt):
        rows = slice(vt * SUBLANES, (vt + 1) * SUBLANES)
        return column_sum([ref[rows, t * LANES : (t + 1) * LANES] for t in range(tiles)])

    pivot_total = totals(pivots_ref, 0)
    own_row = row_of([(vt * SUBLANES, totals(own_ref, vt)) for vt in range(v_tiles)])
    lane = lax.broadcasted_iota(jnp.int32, (SUBLANES, LANES), 1)
    for vt in range(v_tiles):
        partner_row = row_of(
            [(row_count + s * SUBLANES, totals(partner_refs[s], vt)) for s in range(STEPS)]
        )
        rows = jnp.where(lane < row_count, own_row + pivot_total, partner_row)
        for q in range(pivot_count):
            at = (q * v_tiles + vt) * SHARE_ROWS + SUBLANES
            out_ref[at : at + 1, :] = rows[q : q + 1, :]


def quotient_kernel(arrived_ref, out_ref):
    steps, _, row_count = out_ref.shape
    peers = arrived_ref.shape[0] // SHARE_ROWS
    numerator = arrived_ref[0:SUBLANES, :]
    total = arrived_ref[SUBLANES : SUBLANES + 1, :]
    for peer in range(1, peers):
        at = peer * SHARE_ROWS
        numerator = numerator + arrived_ref[at : at + SUBLANES, :]
        total = total + arrived_ref[at + SUBLANES : at + SUBLANES + 1, :]
    totals = jnp.broadcast_to(total, (SUBLANES, LANES))
    for s in range(steps):
        partner = jnp.sum(
            jnp.where(lane_at(row_count + s * SUBLANES), totals, 0.0), axis=1, keepdims=True
        )
        own = totals[:, :row_count]
        part = numerator[:, s * row_count : (s + 1) * row_count]
        out_ref[s] = 1.5 * part / (own + partner)


def in_vmem(array):
    return pltpu.with_memory_space_constraint(array, pltpu.VMEM)


def body(vectors, pivot_ids):
    row_count, width = vectors.shape
    pivot_count = pivot_ids.shape[0]
    wide = lax.axis_size("wide")
    fields = lax.axis_size("fields")
    smem = pl.BlockSpec(memory_space=pltpu.SMEM)
    vmem = pl.BlockSpec(memory_space=pltpu.VMEM)
    copies = pl.pallas_call(
        spread_kernel,
        out_shape=pltpu.VMEM((wide, pivot_count, width), jnp.float32),
        in_specs=[smem, vmem],
        out_specs=vmem,
        scratch_shapes=[pltpu.VMEM((pivot_count, width), jnp.float32)],
        name="spread",
    )(pivot_ids, in_vmem(vectors))
    arrived = to_everyone(copies, "wide")
    partners = [from_behind(vectors, "wide", s) for s in range(1, STEPS + 1)]
    table = pl.pallas_call(
        table_kernel,
        out_shape=pltpu.VMEM((fields * SHARE_ROWS, LANES), jnp.float32),
        in_specs=[smem] + [vmem] * (2 + STEPS),
        out_specs=vmem,
        scratch_shapes=[
            pltpu.VMEM((pivot_count, width), jnp.float32),
            pltpu.VMEM((pivot_count * row_count // LANES, width, LANES), jnp.float32),
        ],
        name="table",
    )(pivot_ids, *(in_vmem(a) for a in (vectors, arrived, *partners)))
    shares = to_everyone(table.reshape(fields, 1, SHARE_ROWS * LANES), "fields")
    quotient = pl.pallas_call(
        quotient_kernel,
        out_shape=jax.ShapeDtypeStruct((STEPS, SUBLANES, row_count), jnp.float32),
        in_specs=[vmem],
        out_specs=vmem,
        name="quotient",
    )(in_vmem(shares.reshape(fields * SHARE_ROWS, LANES)))
    return jnp.transpose(quotient, (2, 0, 1))


def solution(mesh):
    placed = (P("wide", "fields"), P())
    return jax.shard_map(
        body, mesh=mesh, in_specs=placed, out_specs=P("wide", None, "fields"), check_vma=False
    )
```

```python
import jax
import jax.numpy as jnp
from jax import lax
from jax.experimental import pallas as pl
from jax.experimental.pallas import tpu as pltpu
from jax.sharding import PartitionSpec as P

STEPS = 4
UNROLL = 32
LANES = 128
SUBLANES = 8
SHARE_ROWS = SUBLANES + 1


def from_behind(value, axis, steps):
    count = lax.axis_size(axis)
    pairs = [(source, (source + steps) % count) for source in range(count)]
    return lax.ppermute(value, axis, pairs)


def to_everyone(copies, axis):
    return lax.all_to_all(copies, axis, split_axis=0, concat_axis=0, tiled=True)


def spread_kernel(ids_ref, vectors_ref, copies_ref, rows_ref):
    row_count = vectors_ref.shape[0]
    for q in range(rows_ref.shape[0]):
        rows_ref[q : q + 1, :] = vectors_ref[pl.ds(lax.rem(ids_ref[q], row_count), 1), :]
    rows = rows_ref[...]
    for peer in range(copies_ref.shape[0]):
        copies_ref[peer] = rows


def lane_at(offset):
    lane = lax.broadcasted_iota(jnp.int32, (SUBLANES, LANES), 1)
    sublane = lax.broadcasted_iota(jnp.int32, (SUBLANES, LANES), 0)
    return lane == sublane + offset


def column_sum(tiles):
    folded = tiles[0]
    for tile in tiles[1:]:
        folded = folded + tile
    return jnp.sum(folded, axis=1, keepdims=True)


def by_group(columns):
    lane = lax.broadcasted_iota(jnp.int32, (SUBLANES, LANES), 1)
    size = LANES // len(columns)
    tile = jnp.broadcast_to(columns[-1], (SUBLANES, LANES))
    for g in range(len(columns) - 2, -1, -1):
        tile = jnp.where(lane < (g + 1) * size, columns[g], tile)
    return tile


def every_row(ref, row):
    return jnp.broadcast_to(ref[pl.ds(row, 1), :], (SUBLANES, LANES))


def turn_kernel(own_ref, turned_ref):
    row_count, width = own_ref.shape
    for t in range(width // LANES):
        at = slice(t * LANES, (t + 1) * LANES)
        for a in range(SUBLANES):
            rows = jnp.concatenate(
                [
                    jnp.broadcast_to(own_ref[v : v + 1, at], (row_count, LANES))
                    for v in range(a, row_count, SUBLANES)
                ],
                axis=0,
            )
            turned_ref[pl.ds(t * LANES * SUBLANES + a, LANES, stride=SUBLANES), :] = rows.T


def table_kernel(ids_ref, own_ref, turned_ref, arrived_ref, *refs):
    partner_refs = refs[:STEPS]
    out_ref, pivots_ref, fields_ref, splat_ref = refs[STEPS:]
    row_count, width = own_ref.shape
    pivot_count = pivots_ref.shape[0]
    tiles = width // LANES
    groups = row_count // SUBLANES
    for q in range(pivot_count):
        pivots_ref[q : q + 1, :] = arrived_ref[lax.div(ids_ref[q], row_count), q : q + 1, :]

    for t in range(tiles):
        at = slice(t * LANES, (t + 1) * LANES)
        for cg in range(groups):
            rows = [ref[cg * SUBLANES : (cg + 1) * SUBLANES, at] for ref in partner_refs]
            fields_ref[cg * width + t * LANES : cg * width + (t + 1) * LANES, :] = jnp.concatenate(
                rows * groups, axis=0
            ).T
        for q in range(pivot_count):
            splat_ref[q * width + t * LANES : q * width + (t + 1) * LANES, :] = jnp.broadcast_to(
                pivots_ref[q : q + 1, at], (LANES, LANES)
            ).T

    def some_fields(step, sums):
        sums = list(sums)
        for i in range(UNROLL):
            f = step * UNROLL + i
            own = turned_ref[pl.ds(f * SUBLANES, SUBLANES), :]
            partners = [every_row(fields_ref, cg * width + f) for cg in range(groups)]
            for q in range(pivot_count):
                larger = jnp.maximum(own, every_row(splat_ref, q * width + f))
                for cg in range(groups):
                    k = q * groups + cg
                    sums[k] = sums[k] + jnp.minimum(larger, partners[cg])
        return tuple(sums)

    first = []
    for q in range(pivot_count):
        smaller = by_group(
            [
                column_sum(
                    [
                        jnp.minimum(
                            own_ref[g * SUBLANES : (g + 1) * SUBLANES, t * LANES : (t + 1) * LANES],
                            pivots_ref[q : q + 1, t * LANES : (t + 1) * LANES],
                        )
                        for t in range(tiles)
                    ]
                )
                for g in range(groups)
            ]
        )
        first.extend([smaller] * groups)
    sums = lax.fori_loop(0, width // UNROLL, some_fields, tuple(first))

    def totals(ref, g):
        rows = slice(g * SUBLANES, (g + 1) * SUBLANES)
        return column_sum([ref[rows, t * LANES : (t + 1) * LANES] for t in range(tiles)])

    own_row = jnp.zeros((SUBLANES, LANES), jnp.float32)
    for g in range(groups):
        own_row = own_row + jnp.where(lane_at(row_count + g * SUBLANES), totals(own_ref, g), 0.0)
    own_row = jnp.sum(own_row, axis=0, keepdims=True) + totals(pivots_ref, 0)
    lane = lax.broadcasted_iota(jnp.int32, (SUBLANES, LANES), 1)
    for cg in range(groups):
        partner_row = jnp.sum(fields_ref[cg * width : (cg + 1) * width, :], axis=0, keepdims=True)
        rows = jnp.where(lane < STEPS * SUBLANES, partner_row, own_row)
        for q in range(pivot_count):
            at = (q * groups + cg) * SHARE_ROWS
            out_ref[at : at + SUBLANES, :] = sums[q * groups + cg]
            out_ref[at + SUBLANES : at + SUBLANES + 1, :] = rows[q : q + 1, :]


def quotient_kernel(arrived_ref, out_ref):
    steps, _, row_count = out_ref.shape
    peers = arrived_ref.shape[0] // SHARE_ROWS
    groups = row_count // SUBLANES
    size = LANES // groups
    numerator = arrived_ref[0:SUBLANES, :]
    total = arrived_ref[SUBLANES : SUBLANES + 1, :]
    for peer in range(1, peers):
        at = peer * SHARE_ROWS
        numerator = numerator + arrived_ref[at : at + SUBLANES, :]
        total = total + arrived_ref[at + SUBLANES : at + SUBLANES + 1, :]
    totals = jnp.broadcast_to(total, (SUBLANES, LANES))
    own = by_group(
        [
            jnp.sum(jnp.where(lane_at(size + g * SUBLANES), totals, 0.0), axis=1, keepdims=True)
            for g in range(groups)
        ]
    )
    partner = jnp.concatenate([totals[:, :size]] * groups, axis=1)
    turned = (1.5 * numerator / (own + partner)).T
    for s in range(steps):
        rows = [g * size + s * SUBLANES for g in range(groups)]
        out_ref[s] = jnp.concatenate([turned[r : r + SUBLANES, :] for r in rows], axis=1)


def in_vmem(array):
    return pltpu.with_memory_space_constraint(array, pltpu.VMEM)


def body(vectors, pivot_ids):
    row_count, width = vectors.shape
    pivot_count = pivot_ids.shape[0]
    wide = lax.axis_size("wide")
    fields = lax.axis_size("fields")
    smem = pl.BlockSpec(memory_space=pltpu.SMEM)
    vmem = pl.BlockSpec(memory_space=pltpu.VMEM)
    copies = pl.pallas_call(
        spread_kernel,
        out_shape=pltpu.VMEM((wide, pivot_count, width), jnp.float32),
        in_specs=[smem, vmem],
        out_specs=vmem,
        scratch_shapes=[pltpu.VMEM((pivot_count, width), jnp.float32)],
        name="spread",
    )(pivot_ids, in_vmem(vectors))
    arrived = to_everyone(copies, "wide")
    partners = [from_behind(vectors, "wide", s) for s in range(1, STEPS + 1)]
    turned = pl.pallas_call(
        turn_kernel,
        out_shape=pltpu.VMEM((width * SUBLANES, LANES), jnp.float32),
        in_specs=[vmem],
        out_specs=vmem,
        name="turn",
    )(in_vmem(vectors))
    table = pl.pallas_call(
        table_kernel,
        out_shape=pltpu.VMEM((fields * SHARE_ROWS, LANES), jnp.float32),
        in_specs=[smem] + [vmem] * (3 + STEPS),
        out_specs=vmem,
        scratch_shapes=[
            pltpu.VMEM((pivot_count, width), jnp.float32),
            pltpu.VMEM((row_count // SUBLANES * width, LANES), jnp.float32),
            pltpu.VMEM((pivot_count * width, LANES), jnp.float32),
        ],
        name="table",
    )(pivot_ids, *(in_vmem(a) for a in (vectors, turned, arrived, *partners)))
    shares = to_everyone(table.reshape(fields, 1, SHARE_ROWS * LANES), "fields")
    quotient = pl.pallas_call(
        quotient_kernel,
        out_shape=jax.ShapeDtypeStruct((STEPS, SUBLANES, row_count), jnp.float32),
        in_specs=[vmem],
        out_specs=vmem,
        name="quotient",
    )(in_vmem(shares.reshape(fields * SHARE_ROWS, LANES)))
    return jnp.transpose(quotient, (2, 0, 1))


def solution(mesh):
    placed = (P("wide", "fields"), P())
    return jax.shard_map(
        body, mesh=mesh, in_specs=placed, out_specs=P("wide", None, "fields"), check_vma=False
    )
```

```python
import jax
import jax.numpy as jnp
from jax import lax
from jax.experimental import pallas as pl
from jax.experimental.pallas import tpu as pltpu
from jax.sharding import PartitionSpec as P


STEPS = 4
UNROLL = 32
HALVES = 2
LANES = 128
SUBLANES = 8
SHARE_ROWS = SUBLANES + 2


def from_behind(value, axis, steps):
    count = lax.axis_size(axis)
    pairs = [(source, (source + steps) % count) for source in range(count)]
    return lax.ppermute(value, axis, pairs)


def to_everyone(copies, axis):
    return lax.all_to_all(copies, axis, split_axis=0, concat_axis=0, tiled=True)


def spread_kernel(ids_ref, vectors_ref, copies_ref, own_ref, rows_ref):
    row_count = vectors_ref.shape[0]
    for q in range(rows_ref.shape[0]):
        rows_ref[q : q + 1, :] = vectors_ref[pl.ds(lax.rem(ids_ref[q], row_count), 1), :]
    rows = rows_ref[...]
    for peer in range(copies_ref.shape[0]):
        copies_ref[peer] = rows
    own_ref[...] = vectors_ref[...]


def lane_at(offset):
    lane = lax.broadcasted_iota(jnp.int32, (SUBLANES, LANES), 1)
    sublane = lax.broadcasted_iota(jnp.int32, (SUBLANES, LANES), 0)
    return lane == sublane + offset


def column_sum(tiles):
    folded = tiles[0]
    for tile in tiles[1:]:
        folded = folded + tile
    return jnp.sum(folded, axis=1, keepdims=True)


def by_group(columns):
    lane = lax.broadcasted_iota(jnp.int32, (SUBLANES, LANES), 1)
    size = LANES // len(columns)
    tile = jnp.broadcast_to(columns[-1], (SUBLANES, LANES))
    for g in range(len(columns) - 2, -1, -1):
        tile = jnp.where(lane < (g + 1) * size, columns[g], tile)
    return tile


def every_row(ref, row):
    return jnp.broadcast_to(ref[pl.ds(row, 1), :], (SUBLANES, LANES))


def turn_kernel(own_ref, turned_ref):
    row_count, width = own_ref.shape
    copies = LANES // HALVES * SUBLANES // row_count
    for t in range(width // LANES):
        at = slice(t * LANES, (t + 1) * LANES)
        for a in range(SUBLANES):
            rows = [
                jnp.broadcast_to(own_ref[v : v + 1, at], (copies, LANES))
                for v in range(a, row_count, SUBLANES)
            ]
            turned_ref[pl.ds(t * LANES * SUBLANES + a, LANES, stride=SUBLANES), :] = jnp.concatenate(
                rows * HALVES, axis=0
            ).T


def turn_partners(partner_refs, fields_ref):
    row_count, width = partner_refs[0].shape
    groups = row_count // SUBLANES
    for cp in range(groups // HALVES):
        for t in range(width // LANES):
            at = slice(t * LANES, (t + 1) * LANES)
            rows = []
            for h in range(HALVES):
                first = (cp * HALVES + h) * SUBLANES
                rows.extend([ref[first : first + SUBLANES, at] for ref in partner_refs] * groups)
            fields_ref[cp * width + t * LANES : cp * width + (t + 1) * LANES, :] = jnp.concatenate(
                rows, axis=0
            ).T


def sum_fields(turned_ref, splat_ref, fields_ref, smaller):
    width = turned_ref.shape[0] // SUBLANES
    pairs = fields_ref.shape[0] // width
    pivot_count = len(smaller)

    def some_fields(step, sums):
        sums = list(sums)
        for i in range(UNROLL):
            f = step * UNROLL + i
            own = turned_ref[pl.ds(f * SUBLANES, SUBLANES), :]
            partners = [every_row(fields_ref, cp * width + f) for cp in range(pairs)]
            for q in range(pivot_count):
                larger = jnp.maximum(own, every_row(splat_ref, q * width + f))
                for cp in range(pairs):
                    k = q * pairs + cp
                    sums[k] = sums[k] + jnp.minimum(larger, partners[cp])
        return tuple(sums)

    first = tuple(tile for tile in smaller for _ in range(pairs))
    return lax.fori_loop(0, width // UNROLL, some_fields, first)


def partner_totals(fields_ref, width):
    return [
        jnp.sum(fields_ref[first : first + width, :], axis=0, keepdims=True)
        for first in range(0, fields_ref.shape[0], width)
    ]


def early_kernel(ids_ref, own_ref, turned_ref, arrived_ref, *refs):
    count = STEPS // HALVES
    partner_refs = refs[:count]
    splat_ref, smaller_ref, totals_ref, sums_ref, partners_ref, pivots_ref, fields_ref = refs[count:]
    row_count, width = own_ref.shape
    pivot_count = pivots_ref.shape[0]
    tiles = width // LANES
    groups = row_count // SUBLANES
    for q in range(pivot_count):
        pivots_ref[q : q + 1, :] = arrived_ref[lax.div(ids_ref[q], row_count), q : q + 1, :]
    turn_partners(partner_refs, fields_ref)
    for t in range(tiles):
        for q in range(pivot_count):
            splat_ref[q * width + t * LANES : q * width + (t + 1) * LANES, :] = jnp.broadcast_to(
                pivots_ref[q : q + 1, t * LANES : (t + 1) * LANES], (LANES, LANES)
            ).T
    smaller = []
    for q in range(pivot_count):
        columns = [
            column_sum(
                [
                    jnp.minimum(
                        own_ref[g * SUBLANES : (g + 1) * SUBLANES, t * LANES : (t + 1) * LANES],
                        pivots_ref[q : q + 1, t * LANES : (t + 1) * LANES],
                    )
                    for t in range(tiles)
                ]
            )
            for g in range(groups)
        ]
        smaller.append(by_group(columns * HALVES))
        smaller_ref[q * SUBLANES : (q + 1) * SUBLANES, :] = smaller[-1]
    sums = sum_fields(turned_ref, splat_ref, fields_ref, smaller)
    for k, tile in enumerate(sums):
        sums_ref[k * SUBLANES : (k + 1) * SUBLANES, :] = tile

    def totals(ref, g):
        rows = slice(g * SUBLANES, (g + 1) * SUBLANES)
        return column_sum([ref[rows, t * LANES : (t + 1) * LANES] for t in range(tiles)])

    own_row = jnp.zeros((SUBLANES, LANES), jnp.float32)
    for g in range(groups):
        own_row = own_row + jnp.where(lane_at(g * SUBLANES), totals(own_ref, g), 0.0)
    totals_ref[...] = jnp.sum(own_row, axis=0, keepdims=True) + totals(pivots_ref, 0)
    for cp, row in enumerate(partner_totals(fields_ref, width)):
        partners_ref[cp * SUBLANES : (cp + 1) * SUBLANES, :] = jnp.broadcast_to(row, (SUBLANES, LANES))


def late_kernel(turned_ref, splat_ref, smaller_ref, totals_ref, sums_ref, partners_ref, *refs):
    count = STEPS // HALVES
    partner_refs = refs[:count]
    out_ref, fields_ref = refs[count:]
    row_count, width = partner_refs[0].shape
    groups = row_count // SUBLANES
    pairs = groups // HALVES
    pivot_count = smaller_ref.shape[0] // SUBLANES
    turn_partners(partner_refs, fields_ref)
    smaller = [smaller_ref[q * SUBLANES : (q + 1) * SUBLANES, :] for q in range(pivot_count)]
    sums = sum_fields(turned_ref, splat_ref, fields_ref, smaller)

    lane = lax.broadcasted_iota(jnp.int32, (SUBLANES, LANES), 1)
    half = LANES // HALVES

    def joined(early, late):
        return (
            jnp.where(lane < half, early, pltpu.roll(late, half, 1)),
            jnp.where(lane < half, pltpu.roll(early, half, 1), late),
        )

    partners = [
        joined(
            partners_ref[cp * SUBLANES : (cp + 1) * SUBLANES, :],
            jnp.broadcast_to(row, (SUBLANES, LANES)),
        )
        for cp, row in enumerate(partner_totals(fields_ref, width))
    ]
    for q in range(pivot_count):
        for cp in range(pairs):
            k = q * pairs + cp
            tiles = joined(sums_ref[k * SUBLANES : (k + 1) * SUBLANES, :], sums[k])
            for h in range(HALVES):
                at = (k * HALVES + h) * SHARE_ROWS
                out_ref[at : at + SUBLANES, :] = tiles[h]
                out_ref[at + SUBLANES : at + SUBLANES + 1, :] = partners[cp][h][:1, :]
                out_ref[at + SUBLANES + 1 : at + SUBLANES + 2, :] = totals_ref[q : q + 1, :]


def quotient_kernel(arrived_ref, out_ref):
    steps, _, row_count = out_ref.shape
    peers = arrived_ref.shape[0] // SHARE_ROWS
    groups = row_count // SUBLANES
    count = steps // HALVES
    share = arrived_ref[0:SUBLANES, :], arrived_ref[SUBLANES:SHARE_ROWS, :]
    for peer in range(1, peers):
        at = peer * SHARE_ROWS
        share = (
            share[0] + arrived_ref[at : at + SUBLANES, :],
            share[1] + arrived_ref[at + SUBLANES : at + SHARE_ROWS, :],
        )
    numerator, totals = share
    row = jnp.broadcast_to(totals[1:2, :], (SUBLANES, LANES))
    columns = [
        jnp.sum(jnp.where(lane_at(g * SUBLANES), row, 0.0), axis=1, keepdims=True) for g in range(groups)
    ]
    turned = (1.5 * numerator / (by_group(columns * HALVES) + totals[0:1, :])).T
    for s in range(steps):
        k, i = divmod(s, count)
        rows = [(k * groups + g) * count * SUBLANES + i * SUBLANES for g in range(groups)]
        out_ref[s] = jnp.concatenate([turned[r : r + SUBLANES, :] for r in rows], axis=1)


def in_vmem(array):
    return pltpu.with_memory_space_constraint(array, pltpu.VMEM)


def body(vectors, pivot_ids):
    row_count, width = vectors.shape
    pivot_count = pivot_ids.shape[0]
    wide = lax.axis_size("wide")
    fields = lax.axis_size("fields")
    pairs = row_count // SUBLANES // HALVES
    count = STEPS // HALVES
    smem = pl.BlockSpec(memory_space=pltpu.SMEM)
    vmem = pl.BlockSpec(memory_space=pltpu.VMEM)
    small = pltpu.CompilerParams(vmem_limit_bytes=16 << 20)
    copies, vectors = pl.pallas_call(
        spread_kernel,
        out_shape=[
            jax.ShapeDtypeStruct((wide, pivot_count, width), jnp.float32),
            pltpu.VMEM(vectors.shape, jnp.float32),
        ],
        in_specs=[smem, vmem],
        out_specs=[vmem, vmem],
        scratch_shapes=[pltpu.VMEM((pivot_count, width), jnp.float32)],
        name="spread",
    )(pivot_ids, vectors)
    arrived = to_everyone(copies, "wide")
    partners = []
    for s in range(1, STEPS + 1):
        partners.append(in_vmem(from_behind(vectors, "wide", s)))
    turned = pl.pallas_call(
        turn_kernel,
        out_shape=pltpu.VMEM((width * SUBLANES, LANES), jnp.float32),
        in_specs=[vmem],
        out_specs=vmem,
        compiler_params=small,
        name="turn",
    )(in_vmem(vectors))
    between = pl.pallas_call(
        early_kernel,
        out_shape=[
            pltpu.VMEM((pivot_count * width, LANES), jnp.float32),
            pltpu.VMEM((pivot_count * SUBLANES, LANES), jnp.float32),
            pltpu.VMEM((pivot_count, LANES), jnp.float32),
            pltpu.VMEM((pivot_count * pairs * SUBLANES, LANES), jnp.float32),
            pltpu.VMEM((pairs * SUBLANES, LANES), jnp.float32),
        ],
        in_specs=[smem] + [vmem] * (3 + count),
        out_specs=[vmem] * 5,
        scratch_shapes=[
            pltpu.VMEM((pivot_count, width), jnp.float32),
            pltpu.VMEM((pairs * width, LANES), jnp.float32),
        ],
        compiler_params=small,
        name="early",
    )(pivot_ids, in_vmem(vectors), in_vmem(turned), in_vmem(arrived), *partners[:count])
    table = pl.pallas_call(
        late_kernel,
        out_shape=pltpu.VMEM((fields * SHARE_ROWS, LANES), jnp.float32),
        in_specs=[vmem] * (6 + count),
        out_specs=vmem,
        scratch_shapes=[pltpu.VMEM((pairs * width, LANES), jnp.float32)],
        compiler_params=small,
        name="late",
    )(in_vmem(turned), *(in_vmem(a) for a in between), *partners[count:])
    shares = to_everyone(table.reshape(fields, 1, SHARE_ROWS * LANES), "fields")
    quotient = pl.pallas_call(
        quotient_kernel,
        out_shape=jax.ShapeDtypeStruct((STEPS, SUBLANES, row_count), jnp.float32),
        in_specs=[vmem],
        out_specs=vmem,
        name="quotient",
    )(in_vmem(shares.reshape(fields * SHARE_ROWS, LANES)))
    return jnp.transpose(quotient, (2, 0, 1))


def solution(mesh):
    placed = (P("wide", "fields"), P())
    return jax.shard_map(
        body, mesh=mesh, in_specs=placed, out_specs=P("wide", None, "fields"), check_vma=False
    )
```

```python
import jax
import jax.numpy as jnp
from jax import lax
from jax.experimental import pallas as pl
from jax.experimental.pallas import tpu as pltpu
from jax.sharding import PartitionSpec as P


STEPS = 4
UNROLL = 32
HALVES = 2
ORDER = (1, 4), (2, 3)
LANES = 128
SUBLANES = 8
SHARE_ROWS = SUBLANES + 2


def from_behind(value, axis, steps):
    count = lax.axis_size(axis)
    pairs = [(source, (source + steps) % count) for source in range(count)]
    return lax.ppermute(value, axis, pairs)


def to_everyone(copies, axis):
    return lax.all_to_all(copies, axis, split_axis=0, concat_axis=0, tiled=True)


def spread_kernel(ids_ref, vectors_ref, copies_ref, own_ref, rows_ref):
    row_count = vectors_ref.shape[0]
    for q in range(rows_ref.shape[0]):
        rows_ref[q : q + 1, :] = vectors_ref[pl.ds(lax.rem(ids_ref[q], row_count), 1), :]
    rows = rows_ref[...]
    for peer in range(copies_ref.shape[0]):
        copies_ref[peer] = rows
    own_ref[...] = vectors_ref[...]


def lane_at(offset):
    lane = lax.broadcasted_iota(jnp.int32, (SUBLANES, LANES), 1)
    sublane = lax.broadcasted_iota(jnp.int32, (SUBLANES, LANES), 0)
    return lane == sublane + offset


def column_sum(tiles):
    folded = tiles[0]
    for tile in tiles[1:]:
        folded = folded + tile
    return jnp.sum(folded, axis=1, keepdims=True)


def by_group(columns):
    lane = lax.broadcasted_iota(jnp.int32, (SUBLANES, LANES), 1)
    size = LANES // len(columns)
    tile = jnp.broadcast_to(columns[-1], (SUBLANES, LANES))
    for g in range(len(columns) - 2, -1, -1):
        tile = jnp.where(lane < (g + 1) * size, columns[g], tile)
    return tile


def every_row(ref, row):
    return jnp.broadcast_to(ref[pl.ds(row, 1), :], (SUBLANES, LANES))


def turn_kernel(own_ref, turned_ref):
    row_count, width = own_ref.shape
    copies = LANES // HALVES * SUBLANES // row_count
    for t in range(width // LANES):
        at = slice(t * LANES, (t + 1) * LANES)
        for a in range(SUBLANES):
            rows = [
                jnp.broadcast_to(own_ref[v : v + 1, at], (copies, LANES))
                for v in range(a, row_count, SUBLANES)
            ]
            turned_ref[pl.ds(t * LANES * SUBLANES + a, LANES, stride=SUBLANES), :] = jnp.concatenate(
                rows * HALVES, axis=0
            ).T


def turn_partners(partners, fields_ref, row_count):
    width = partners[0][0].shape[1]
    groups = row_count // SUBLANES
    for cp in range(groups // HALVES):
        for t in range(width // LANES):
            at = slice(t * LANES, (t + 1) * LANES)
            rows = []
            for h in range(HALVES):
                first = (cp * HALVES + h) * SUBLANES
                rows.extend(
                    [ref[base + first : base + first + SUBLANES, at] for ref, base in partners] * groups
                )
            fields_ref[cp * width + t * LANES : cp * width + (t + 1) * LANES, :] = jnp.concatenate(
                rows, axis=0
            ).T


def sum_fields(turned_ref, splat_ref, fields_ref, smaller):
    width = turned_ref.shape[0] // SUBLANES
    pairs = fields_ref.shape[0] // width
    pivot_count = len(smaller)

    def some_fields(step, sums):
        sums = list(sums)
        for i in range(UNROLL):
            f = step * UNROLL + i
            own = turned_ref[pl.ds(f * SUBLANES, SUBLANES), :]
            partners = [every_row(fields_ref, cp * width + f) for cp in range(pairs)]
            for q in range(pivot_count):
                larger = jnp.maximum(own, every_row(splat_ref, q * width + f))
                for cp in range(pairs):
                    k = q * pairs + cp
                    sums[k] = sums[k] + jnp.minimum(larger, partners[cp])
        return tuple(sums)

    first = tuple(tile for tile in smaller for _ in range(pairs))
    return lax.fori_loop(0, width // UNROLL, some_fields, first)


def partner_totals(fields_ref, width):
    return [
        jnp.sum(fields_ref[first : first + width, :], axis=0, keepdims=True)
        for first in range(0, fields_ref.shape[0], width)
    ]


def early_kernel(ids_ref, own_ref, turned_ref, arrived_ref, *refs):
    count = STEPS // HALVES
    partner_refs = refs[:count]
    splat_ref, smaller_ref, totals_ref, sums_ref, partners_ref, pivots_ref, fields_ref = refs[count:]
    row_count, width = own_ref.shape
    pivot_count = pivots_ref.shape[0]
    tiles = width // LANES
    groups = row_count // SUBLANES
    for q in range(pivot_count):
        pivots_ref[q : q + 1, :] = arrived_ref[lax.div(ids_ref[q], row_count), q : q + 1, :]
    turn_partners([(ref, 0) for ref in partner_refs], fields_ref, row_count)
    for t in range(tiles):
        for q in range(pivot_count):
            splat_ref[q * width + t * LANES : q * width + (t + 1) * LANES, :] = jnp.broadcast_to(
                pivots_ref[q : q + 1, t * LANES : (t + 1) * LANES], (LANES, LANES)
            ).T
    smaller = []
    for q in range(pivot_count):
        columns = [
            column_sum(
                [
                    jnp.minimum(
                        own_ref[g * SUBLANES : (g + 1) * SUBLANES, t * LANES : (t + 1) * LANES],
                        pivots_ref[q : q + 1, t * LANES : (t + 1) * LANES],
                    )
                    for t in range(tiles)
                ]
            )
            for g in range(groups)
        ]
        smaller.append(by_group(columns * HALVES))
        smaller_ref[q * SUBLANES : (q + 1) * SUBLANES, :] = smaller[-1]
    sums = sum_fields(turned_ref, splat_ref, fields_ref, smaller)
    for k, tile in enumerate(sums):
        sums_ref[k * SUBLANES : (k + 1) * SUBLANES, :] = tile

    def totals(ref, g):
        rows = slice(g * SUBLANES, (g + 1) * SUBLANES)
        return column_sum([ref[rows, t * LANES : (t + 1) * LANES] for t in range(tiles)])

    own_row = jnp.zeros((SUBLANES, LANES), jnp.float32)
    for g in range(groups):
        own_row = own_row + jnp.where(lane_at(g * SUBLANES), totals(own_ref, g), 0.0)
    totals_ref[...] = jnp.sum(own_row, axis=0, keepdims=True) + totals(pivots_ref, 0)
    for cp, row in enumerate(partner_totals(fields_ref, width)):
        partners_ref[cp * SUBLANES : (cp + 1) * SUBLANES, :] = jnp.broadcast_to(row, (SUBLANES, LANES))


def late_kernel(
    turned_ref, splat_ref, smaller_ref, totals_ref, sums_ref, partners_ref, pair_ref, out_ref, fields_ref
):
    width = pair_ref.shape[1]
    row_count = pair_ref.shape[0] // HALVES
    groups = row_count // SUBLANES
    pairs = groups // HALVES
    pivot_count = smaller_ref.shape[0] // SUBLANES
    turn_partners([(pair_ref, 0), (pair_ref, row_count)], fields_ref, row_count)
    smaller = [smaller_ref[q * SUBLANES : (q + 1) * SUBLANES, :] for q in range(pivot_count)]
    sums = sum_fields(turned_ref, splat_ref, fields_ref, smaller)

    lane = lax.broadcasted_iota(jnp.int32, (SUBLANES, LANES), 1)
    half = LANES // HALVES

    def joined(early, late):
        return (
            jnp.where(lane < half, early, pltpu.roll(late, half, 1)),
            jnp.where(lane < half, pltpu.roll(early, half, 1), late),
        )

    partners = [
        joined(
            partners_ref[cp * SUBLANES : (cp + 1) * SUBLANES, :],
            jnp.broadcast_to(row, (SUBLANES, LANES)),
        )
        for cp, row in enumerate(partner_totals(fields_ref, width))
    ]
    for q in range(pivot_count):
        for cp in range(pairs):
            k = q * pairs + cp
            tiles = joined(sums_ref[k * SUBLANES : (k + 1) * SUBLANES, :], sums[k])
            for h in range(HALVES):
                at = (k * HALVES + h) * SHARE_ROWS
                out_ref[at : at + SUBLANES, :] = tiles[h]
                out_ref[at + SUBLANES : at + SUBLANES + 1, :] = partners[cp][h][:1, :]
                out_ref[at + SUBLANES + 1 : at + SUBLANES + 2, :] = totals_ref[q : q + 1, :]


def quotient_kernel(arrived_ref, out_ref):
    steps, _, row_count = out_ref.shape
    peers = arrived_ref.shape[0] // SHARE_ROWS
    groups = row_count // SUBLANES
    count = steps // HALVES
    share = arrived_ref[0:SUBLANES, :], arrived_ref[SUBLANES:SHARE_ROWS, :]
    for peer in range(1, peers):
        at = peer * SHARE_ROWS
        share = (
            share[0] + arrived_ref[at : at + SUBLANES, :],
            share[1] + arrived_ref[at + SUBLANES : at + SHARE_ROWS, :],
        )
    numerator, totals = share
    row = jnp.broadcast_to(totals[1:2, :], (SUBLANES, LANES))
    columns = [
        jnp.sum(jnp.where(lane_at(g * SUBLANES), row, 0.0), axis=1, keepdims=True) for g in range(groups)
    ]
    turned = (1.5 * numerator / (by_group(columns * HALVES) + totals[0:1, :])).T
    for s in range(steps):
        k, i = next((k, half.index(s + 1)) for k, half in enumerate(ORDER) if s + 1 in half)
        rows = [(k * groups + g) * count * SUBLANES + i * SUBLANES for g in range(groups)]
        out_ref[s] = jnp.concatenate([turned[r : r + SUBLANES, :] for r in rows], axis=1)


def in_vmem(array):
    return pltpu.with_memory_space_constraint(array, pltpu.VMEM)


def body(vectors, pivot_ids):
    row_count, width = vectors.shape
    pivot_count = pivot_ids.shape[0]
    wide = lax.axis_size("wide")
    fields = lax.axis_size("fields")
    pairs = row_count // SUBLANES // HALVES
    count = STEPS // HALVES
    smem = pl.BlockSpec(memory_space=pltpu.SMEM)
    vmem = pl.BlockSpec(memory_space=pltpu.VMEM)
    small = pltpu.CompilerParams(vmem_limit_bytes=16 << 20)
    copies, vectors = pl.pallas_call(
        spread_kernel,
        out_shape=[
            jax.ShapeDtypeStruct((wide, pivot_count, width), jnp.float32),
            pltpu.VMEM(vectors.shape, jnp.float32),
        ],
        in_specs=[smem, vmem],
        out_specs=[vmem, vmem],
        scratch_shapes=[pltpu.VMEM((pivot_count, width), jnp.float32)],
        name="spread",
    )(pivot_ids, vectors)
    arrived = to_everyone(copies, "wide")
    behind = from_behind(vectors, "wide", 1)
    pair = from_behind(jnp.concatenate([vectors, behind]), "wide", 2)
    farthest = from_behind(vectors, "wide", STEPS)
    turned = pl.pallas_call(
        turn_kernel,
        out_shape=pltpu.VMEM((width * SUBLANES, LANES), jnp.float32),
        in_specs=[vmem],
        out_specs=vmem,
        compiler_params=small,
        name="turn",
    )(in_vmem(vectors))
    between = pl.pallas_call(
        early_kernel,
        out_shape=[
            pltpu.VMEM((pivot_count * width, LANES), jnp.float32),
            pltpu.VMEM((pivot_count * SUBLANES, LANES), jnp.float32),
            pltpu.VMEM((pivot_count, LANES), jnp.float32),
            pltpu.VMEM((pivot_count * pairs * SUBLANES, LANES), jnp.float32),
            pltpu.VMEM((pairs * SUBLANES, LANES), jnp.float32),
        ],
        in_specs=[smem] + [vmem] * (3 + count),
        out_specs=[vmem] * 5,
        scratch_shapes=[pltpu.VMEM((pivot_count, width), jnp.float32), pltpu.VMEM((pairs * width, LANES), jnp.float32)],
        compiler_params=small,
        name="early",
    )(pivot_ids, in_vmem(vectors), in_vmem(turned), *(in_vmem(a) for a in (arrived, behind, farthest)))
    table = pl.pallas_call(
        late_kernel,
        out_shape=pltpu.VMEM((fields * SHARE_ROWS, LANES), jnp.float32),
        in_specs=[vmem] * 7,
        out_specs=vmem,
        scratch_shapes=[pltpu.VMEM((pairs * width, LANES), jnp.float32)],
        compiler_params=small,
        name="late",
    )(in_vmem(turned), *(in_vmem(a) for a in (*between, pair)))
    shares = to_everyone(table.reshape(fields, 1, SHARE_ROWS * LANES), "fields")
    quotient = pl.pallas_call(
        quotient_kernel,
        out_shape=jax.ShapeDtypeStruct((STEPS, SUBLANES, row_count), jnp.float32),
        in_specs=[vmem],
        out_specs=vmem,
        name="quotient",
    )(in_vmem(shares.reshape(fields * SHARE_ROWS, LANES)))
    return jnp.transpose(quotient, (2, 0, 1))


def solution(mesh):
    placed = (P("wide", "fields"), P())
    return jax.shard_map(
        body, mesh=mesh, in_specs=placed, out_specs=P("wide", None, "fields"), check_vma=False
    )
```

```python
import jax
import jax.numpy as jnp
from jax import lax
from jax.experimental import pallas as pl
from jax.experimental.pallas import tpu as pltpu
from jax.sharding import PartitionSpec as P


STEPS = 4
UNROLL = 32
LANES = 128
SUBLANES = 8
SHARE_ROWS = SUBLANES + 1


def from_behind(value, axis, steps):
    count = lax.axis_size(axis)
    pairs = [(source, (source + steps) % count) for source in range(count)]
    return lax.ppermute(value, axis, pairs)


def to_everyone(copies, axis, groups=None):
    return lax.all_to_all(
        copies, axis, split_axis=0, concat_axis=0, tiled=True, axis_index_groups=groups
    )


def block_distance(ids_ref, q, row_count, behind, blocks):
    return lax.rem(behind - lax.div(ids_ref[q], row_count) + blocks, blocks)


def spread_kernel(ids_ref, place_ref, *refs):
    held_refs = refs[:STEPS]
    copies_ref, held_ref, rows_ref = refs[STEPS:]
    row_count = held_refs[0].shape[0]
    blocks = copies_ref.shape[0] * STEPS
    for step, ref in enumerate(held_refs):
        held_ref[step] = ref[...]
    for q in range(rows_ref.shape[0]):
        step = lax.min(block_distance(ids_ref, q, row_count, place_ref[0], blocks), STEPS - 1)
        rows_ref[q : q + 1, :] = held_ref[step, pl.ds(lax.rem(ids_ref[q], row_count), 1), :]
    rows = rows_ref[...]
    for peer in range(copies_ref.shape[0]):
        copies_ref[peer] = rows


def lane_at(offset):
    lane = lax.broadcasted_iota(jnp.int32, (SUBLANES, LANES), 1)
    sublane = lax.broadcasted_iota(jnp.int32, (SUBLANES, LANES), 0)
    return lane == sublane + offset


def column_sum(tiles):
    folded = tiles[0]
    for tile in tiles[1:]:
        folded = folded + tile
    return jnp.sum(folded, axis=1, keepdims=True)


def by_group(columns):
    lane = lax.broadcasted_iota(jnp.int32, (SUBLANES, LANES), 1)
    size = LANES // len(columns)
    tile = jnp.broadcast_to(columns[-1], (SUBLANES, LANES))
    for g in range(len(columns) - 2, -1, -1):
        tile = jnp.where(lane < (g + 1) * size, columns[g], tile)
    return tile


def every_row(ref, row):
    return jnp.broadcast_to(ref[pl.ds(row, 1), :], (SUBLANES, LANES))


def turn_kernel(own_ref, turned_ref):
    row_count, width = own_ref.shape
    for t in range(width // LANES):
        at = slice(t * LANES, (t + 1) * LANES)
        for a in range(SUBLANES):
            rows = jnp.concatenate(
                [
                    jnp.broadcast_to(own_ref[v : v + 1, at], (row_count, LANES))
                    for v in range(a, row_count, SUBLANES)
                ],
                axis=0,
            )
            turned_ref[pl.ds(t * LANES * SUBLANES + a, LANES, stride=SUBLANES), :] = rows.T


def table_kernel(ids_ref, place_ref, own_ref, turned_ref, arrived_ref, *refs):
    partner_refs = refs[:STEPS]
    out_ref, pivots_ref, fields_ref, splat_ref = refs[STEPS:]
    row_count, width = own_ref.shape
    pivot_count = pivots_ref.shape[0]
    tiles = width // LANES
    groups = row_count // SUBLANES
    peers = arrived_ref.shape[0]
    for q in range(pivot_count):
        ahead = lax.div(
            block_distance(ids_ref, q, row_count, place_ref[0], peers * STEPS), STEPS
        )
        peer = lax.rem(lax.div(place_ref[0], STEPS) - ahead + peers, peers)
        pivots_ref[q : q + 1, :] = arrived_ref[peer, q : q + 1, :]

    for t in range(tiles):
        at = slice(t * LANES, (t + 1) * LANES)
        for cg in range(groups):
            rows = [ref[cg * SUBLANES : (cg + 1) * SUBLANES, at] for ref in partner_refs]
            fields_ref[cg * width + t * LANES : cg * width + (t + 1) * LANES, :] = jnp.concatenate(
                rows * groups, axis=0
            ).T
        for q in range(pivot_count):
            splat_ref[q * width + t * LANES : q * width + (t + 1) * LANES, :] = jnp.broadcast_to(
                pivots_ref[q : q + 1, at], (LANES, LANES)
            ).T

    def some_fields(step, sums):
        sums = list(sums)
        for i in range(UNROLL):
            f = step * UNROLL + i
            own = turned_ref[pl.ds(f * SUBLANES, SUBLANES), :]
            partners = [every_row(fields_ref, cg * width + f) for cg in range(groups)]
            for q in range(pivot_count):
                larger = jnp.maximum(own, every_row(splat_ref, q * width + f))
                for cg in range(groups):
                    k = q * groups + cg
                    sums[k] = sums[k] + jnp.minimum(larger, partners[cg])
        return tuple(sums)

    first = []
    for q in range(pivot_count):
        smaller = by_group(
            [
                column_sum(
                    [
                        jnp.minimum(
                            own_ref[g * SUBLANES : (g + 1) * SUBLANES, t * LANES : (t + 1) * LANES],
                            pivots_ref[q : q + 1, t * LANES : (t + 1) * LANES],
                        )
                        for t in range(tiles)
                    ]
                )
                for g in range(groups)
            ]
        )
        first.extend([smaller] * groups)
    sums = lax.fori_loop(0, width // UNROLL, some_fields, tuple(first))

    def totals(ref, g):
        rows = slice(g * SUBLANES, (g + 1) * SUBLANES)
        return column_sum([ref[rows, t * LANES : (t + 1) * LANES] for t in range(tiles)])

    own_row = jnp.zeros((SUBLANES, LANES), jnp.float32)
    for g in range(groups):
        own_row = own_row + jnp.where(lane_at(row_count + g * SUBLANES), totals(own_ref, g), 0.0)
    own_row = jnp.sum(own_row, axis=0, keepdims=True) + totals(pivots_ref, 0)
    lane = lax.broadcasted_iota(jnp.int32, (SUBLANES, LANES), 1)
    for cg in range(groups):
        partner_row = jnp.sum(fields_ref[cg * width : (cg + 1) * width, :], axis=0, keepdims=True)
        rows = jnp.where(lane < STEPS * SUBLANES, partner_row, own_row)
        for q in range(pivot_count):
            at = (q * groups + cg) * SHARE_ROWS
            out_ref[at : at + SUBLANES, :] = sums[q * groups + cg]
            out_ref[at + SUBLANES : at + SUBLANES + 1, :] = rows[q : q + 1, :]


def quotient_kernel(arrived_ref, out_ref):
    steps, _, row_count = out_ref.shape
    peers = arrived_ref.shape[0] // SHARE_ROWS
    groups = row_count // SUBLANES
    size = LANES // groups
    numerator = arrived_ref[0:SUBLANES, :]
    total = arrived_ref[SUBLANES : SUBLANES + 1, :]
    for peer in range(1, peers):
        at = peer * SHARE_ROWS
        numerator = numerator + arrived_ref[at : at + SUBLANES, :]
        total = total + arrived_ref[at + SUBLANES : at + SUBLANES + 1, :]
    totals = jnp.broadcast_to(total, (SUBLANES, LANES))
    own = by_group(
        [
            jnp.sum(jnp.where(lane_at(size + g * SUBLANES), totals, 0.0), axis=1, keepdims=True)
            for g in range(groups)
        ]
    )
    partner = jnp.concatenate([totals[:, :size]] * groups, axis=1)
    turned = (1.5 * numerator / (own + partner)).T
    for s in range(steps):
        rows = [g * size + s * SUBLANES for g in range(groups)]
        out_ref[s] = jnp.concatenate([turned[r : r + SUBLANES, :] for r in rows], axis=1)


def in_vmem(array):
    return pltpu.with_memory_space_constraint(array, pltpu.VMEM)


def body(vectors, pivot_ids):
    row_count, width = vectors.shape
    pivot_count = pivot_ids.shape[0]
    wide = lax.axis_size("wide")
    fields = lax.axis_size("fields")
    smem = pl.BlockSpec(memory_space=pltpu.SMEM)
    vmem = pl.BlockSpec(memory_space=pltpu.VMEM)
    small = pltpu.CompilerParams(vmem_limit_bytes=16 << 20)
    peers = wide // STEPS
    apart = [[first + STEPS * peer for peer in range(peers)] for first in range(STEPS)]
    place = lax.axis_index("wide").astype(jnp.int32).reshape(1)
    partners = []
    for s in range(1, STEPS + 1):
        partners.append(from_behind(vectors, "wide", s))
    turned = pl.pallas_call(
        turn_kernel,
        out_shape=pltpu.VMEM((width * SUBLANES, LANES), jnp.float32),
        in_specs=[vmem],
        out_specs=vmem,
        compiler_params=small,
        name="turn",
    )(in_vmem(vectors))
    copies = pl.pallas_call(
        spread_kernel,
        out_shape=jax.ShapeDtypeStruct((peers, pivot_count, width), jnp.float32),
        in_specs=[smem] * 2 + [vmem] * STEPS,
        out_specs=vmem,
        scratch_shapes=[
            pltpu.VMEM((STEPS, row_count, width), jnp.float32),
            pltpu.VMEM((pivot_count, width), jnp.float32),
        ],
        compiler_params=small,
        name="spread",
    )(pivot_ids, place, *(in_vmem(a) for a in (vectors, *partners[:-1])))
    arrived = to_everyone(copies, "wide", apart)
    table = pl.pallas_call(
        table_kernel,
        out_shape=pltpu.VMEM((fields * SHARE_ROWS, LANES), jnp.float32),
        in_specs=[smem] * 2 + [vmem] * (3 + STEPS),
        out_specs=vmem,
        scratch_shapes=[
            pltpu.VMEM((pivot_count, width), jnp.float32),
            pltpu.VMEM((row_count // SUBLANES * width, LANES), jnp.float32),
            pltpu.VMEM((pivot_count * width, LANES), jnp.float32),
        ],
        compiler_params=small,
        name="table",
    )(pivot_ids, place, *(in_vmem(a) for a in (vectors, turned, arrived, *partners)))
    shares = to_everyone(table.reshape(fields, 1, SHARE_ROWS * LANES), "fields")
    quotient = pl.pallas_call(
        quotient_kernel,
        out_shape=jax.ShapeDtypeStruct((STEPS, SUBLANES, row_count), jnp.float32),
        in_specs=[vmem],
        out_specs=vmem,
        name="quotient",
    )(in_vmem(shares.reshape(fields * SHARE_ROWS, LANES)))
    return jnp.transpose(quotient, (2, 0, 1))


def solution(mesh):
    placed = (P("wide", "fields"), P())
    return jax.shard_map(
        body, mesh=mesh, in_specs=placed, out_specs=P("wide", None, "fields"), check_vma=False
    )
```

```python
import jax
import jax.numpy as jnp
from jax import lax
from jax.experimental import pallas as pl
from jax.experimental.pallas import tpu as pltpu
from jax.sharding import PartitionSpec as P


STEPS = 4
UNROLL = 32
LANES = 128
SUBLANES = 8
SHARE_ROWS = SUBLANES + 1


def from_behind(value, axis, steps):
    count = lax.axis_size(axis)
    pairs = [(source, (source + steps) % count) for source in range(count)]
    return lax.ppermute(value, axis, pairs)


def to_everyone(copies, axis, groups=None):
    return lax.all_to_all(
        copies, axis, split_axis=0, concat_axis=0, tiled=True, axis_index_groups=groups
    )


def block_distance(ids_ref, q, row_count, behind, blocks):
    return lax.rem(behind - lax.div(ids_ref[q], row_count) + blocks, blocks)


def spread_kernel(ids_ref, place_ref, *refs):
    held_refs = refs[:STEPS]
    copies_ref, held_ref, rows_ref = refs[STEPS:]
    row_count = held_refs[0].shape[0]
    blocks = copies_ref.shape[0] * STEPS
    for step, ref in enumerate(held_refs):
        held_ref[step] = ref[...]
    for q in range(rows_ref.shape[0]):
        step = lax.min(block_distance(ids_ref, q, row_count, place_ref[0], blocks), STEPS - 1)
        rows_ref[q : q + 1, :] = held_ref[step, pl.ds(lax.rem(ids_ref[q], row_count), 1), :]
    rows = rows_ref[...]
    for peer in range(copies_ref.shape[0]):
        copies_ref[peer] = rows


def lane_at(offset):
    lane = lax.broadcasted_iota(jnp.int32, (SUBLANES, LANES), 1)
    sublane = lax.broadcasted_iota(jnp.int32, (SUBLANES, LANES), 0)
    return lane == sublane + offset


def column_sum(tiles):
    folded = tiles[0]
    for tile in tiles[1:]:
        folded = folded + tile
    return jnp.sum(folded, axis=1, keepdims=True)


def by_group(columns):
    lane = lax.broadcasted_iota(jnp.int32, (SUBLANES, LANES), 1)
    size = LANES // len(columns)
    tile = jnp.broadcast_to(columns[-1], (SUBLANES, LANES))
    for g in range(len(columns) - 2, -1, -1):
        tile = jnp.where(lane < (g + 1) * size, columns[g], tile)
    return tile


def every_row(ref, row):
    return jnp.broadcast_to(ref[pl.ds(row, 1), :], (SUBLANES, LANES))


def turn_kernel(own_ref, turned_ref):
    row_count, width = own_ref.shape
    for t in range(width // LANES):
        at = slice(t * LANES, (t + 1) * LANES)
        for a in range(SUBLANES):
            rows = jnp.concatenate(
                [
                    jnp.broadcast_to(own_ref[v : v + 1, at], (row_count, LANES))
                    for v in range(a, row_count, SUBLANES)
                ],
                axis=0,
            )
            turned_ref[pl.ds(t * LANES * SUBLANES + a, LANES, stride=SUBLANES), :] = rows.T


def partners_kernel(*refs):
    partner_refs = refs[:STEPS]
    (fields_ref,) = refs[STEPS:]
    row_count, width = partner_refs[0].shape
    groups = row_count // SUBLANES
    for t in range(width // LANES):
        at = slice(t * LANES, (t + 1) * LANES)
        for cg in range(groups):
            rows = [ref[cg * SUBLANES : (cg + 1) * SUBLANES, at] for ref in partner_refs]
            fields_ref[cg * width + t * LANES : cg * width + (t + 1) * LANES, :] = jnp.concatenate(
                rows * groups, axis=0
            ).T


def table_kernel(
    ids_ref, place_ref, own_ref, turned_ref, fields_ref, arrived_ref, out_ref, pivots_ref, splat_ref
):
    row_count, width = own_ref.shape
    pivot_count = pivots_ref.shape[0]
    tiles = width // LANES
    groups = row_count // SUBLANES
    peers = arrived_ref.shape[0]
    for q in range(pivot_count):
        ahead = lax.div(
            block_distance(ids_ref, q, row_count, place_ref[0], peers * STEPS), STEPS
        )
        peer = lax.rem(lax.div(place_ref[0], STEPS) - ahead + peers, peers)
        pivots_ref[q : q + 1, :] = arrived_ref[peer, q : q + 1, :]

    for t in range(tiles):
        at = slice(t * LANES, (t + 1) * LANES)
        for q in range(pivot_count):
            splat_ref[q * width + t * LANES : q * width + (t + 1) * LANES, :] = jnp.broadcast_to(
                pivots_ref[q : q + 1, at], (LANES, LANES)
            ).T

    def some_fields(step, sums):
        sums = list(sums)
        for i in range(UNROLL):
            f = step * UNROLL + i
            own = turned_ref[pl.ds(f * SUBLANES, SUBLANES), :]
            partners = [every_row(fields_ref, cg * width + f) for cg in range(groups)]
            for q in range(pivot_count):
                larger = jnp.maximum(own, every_row(splat_ref, q * width + f))
                for cg in range(groups):
                    k = q * groups + cg
                    sums[k] = sums[k] + jnp.minimum(larger, partners[cg])
        return tuple(sums)

    first = []
    for q in range(pivot_count):
        smaller = by_group(
            [
                column_sum(
                    [
                        jnp.minimum(
                            own_ref[g * SUBLANES : (g + 1) * SUBLANES, t * LANES : (t + 1) * LANES],
                            pivots_ref[q : q + 1, t * LANES : (t + 1) * LANES],
                        )
                        for t in range(tiles)
                    ]
                )
                for g in range(groups)
            ]
        )
        first.extend([smaller] * groups)
    sums = lax.fori_loop(0, width // UNROLL, some_fields, tuple(first))

    def totals(ref, g):
        rows = slice(g * SUBLANES, (g + 1) * SUBLANES)
        return column_sum([ref[rows, t * LANES : (t + 1) * LANES] for t in range(tiles)])

    own_row = jnp.zeros((SUBLANES, LANES), jnp.float32)
    for g in range(groups):
        own_row = own_row + jnp.where(lane_at(row_count + g * SUBLANES), totals(own_ref, g), 0.0)
    own_row = jnp.sum(own_row, axis=0, keepdims=True) + totals(pivots_ref, 0)
    lane = lax.broadcasted_iota(jnp.int32, (SUBLANES, LANES), 1)
    for cg in range(groups):
        partner_row = jnp.sum(fields_ref[cg * width : (cg + 1) * width, :], axis=0, keepdims=True)
        rows = jnp.where(lane < STEPS * SUBLANES, partner_row, own_row)
        for q in range(pivot_count):
            at = (q * groups + cg) * SHARE_ROWS
            out_ref[at : at + SUBLANES, :] = sums[q * groups + cg]
            out_ref[at + SUBLANES : at + SUBLANES + 1, :] = rows[q : q + 1, :]


def quotient_kernel(arrived_ref, out_ref):
    steps, _, row_count = out_ref.shape
    peers = arrived_ref.shape[0] // SHARE_ROWS
    groups = row_count // SUBLANES
    size = LANES // groups
    numerator = arrived_ref[0:SUBLANES, :]
    total = arrived_ref[SUBLANES : SUBLANES + 1, :]
    for peer in range(1, peers):
        at = peer * SHARE_ROWS
        numerator = numerator + arrived_ref[at : at + SUBLANES, :]
        total = total + arrived_ref[at + SUBLANES : at + SUBLANES + 1, :]
    totals = jnp.broadcast_to(total, (SUBLANES, LANES))
    own = by_group(
        [
            jnp.sum(jnp.where(lane_at(size + g * SUBLANES), totals, 0.0), axis=1, keepdims=True)
            for g in range(groups)
        ]
    )
    partner = jnp.concatenate([totals[:, :size]] * groups, axis=1)
    turned = (1.5 * numerator / (own + partner)).T
    for s in range(steps):
        rows = [g * size + s * SUBLANES for g in range(groups)]
        out_ref[s] = jnp.concatenate([turned[r : r + SUBLANES, :] for r in rows], axis=1)


def in_vmem(array):
    return pltpu.with_memory_space_constraint(array, pltpu.VMEM)


def body(vectors, pivot_ids):
    row_count, width = vectors.shape
    pivot_count = pivot_ids.shape[0]
    wide = lax.axis_size("wide")
    fields = lax.axis_size("fields")
    smem = pl.BlockSpec(memory_space=pltpu.SMEM)
    vmem = pl.BlockSpec(memory_space=pltpu.VMEM)
    small = pltpu.CompilerParams(vmem_limit_bytes=16 << 20)
    peers = wide // STEPS
    apart = [[first + STEPS * peer for peer in range(peers)] for first in range(STEPS)]
    place = lax.axis_index("wide").astype(jnp.int32).reshape(1)
    partners = []
    for s in range(1, STEPS + 1):
        partners.append(from_behind(vectors, "wide", s))
    turned = pl.pallas_call(
        turn_kernel,
        out_shape=pltpu.VMEM((width * SUBLANES, LANES), jnp.float32),
        in_specs=[vmem],
        out_specs=vmem,
        compiler_params=small,
        name="turn",
    )(in_vmem(vectors))
    copies = pl.pallas_call(
        spread_kernel,
        out_shape=jax.ShapeDtypeStruct((peers, pivot_count, width), jnp.float32),
        in_specs=[smem] * 2 + [vmem] * STEPS,
        out_specs=vmem,
        scratch_shapes=[
            pltpu.VMEM((STEPS, row_count, width), jnp.float32),
            pltpu.VMEM((pivot_count, width), jnp.float32),
        ],
        compiler_params=small,
        name="spread",
    )(pivot_ids, place, *(in_vmem(a) for a in (vectors, *partners[:-1])))
    arrived = to_everyone(copies, "wide", apart)
    turned_partners = pl.pallas_call(
        partners_kernel,
        out_shape=pltpu.VMEM((row_count // SUBLANES * width, LANES), jnp.float32),
        in_specs=[vmem] * STEPS,
        out_specs=vmem,
        compiler_params=small,
        name="partners",
    )(*(in_vmem(a) for a in partners))
    table = pl.pallas_call(
        table_kernel,
        out_shape=pltpu.VMEM((fields * SHARE_ROWS, LANES), jnp.float32),
        in_specs=[smem] * 2 + [vmem] * 4,
        out_specs=vmem,
        scratch_shapes=[
            pltpu.VMEM((pivot_count, width), jnp.float32),
            pltpu.VMEM((pivot_count * width, LANES), jnp.float32),
        ],
        compiler_params=small,
        name="table",
    )(pivot_ids, place, *(in_vmem(a) for a in (vectors, turned, turned_partners, arrived)))
    shares = to_everyone(table.reshape(fields, 1, SHARE_ROWS * LANES), "fields")
    quotient = pl.pallas_call(
        quotient_kernel,
        out_shape=jax.ShapeDtypeStruct((STEPS, SUBLANES, row_count), jnp.float32),
        in_specs=[vmem],
        out_specs=vmem,
        name="quotient",
    )(in_vmem(shares.reshape(fields * SHARE_ROWS, LANES)))
    return jnp.transpose(quotient, (2, 0, 1))


def solution(mesh):
    placed = (P("wide", "fields"), P())
    return jax.shard_map(
        body, mesh=mesh, in_specs=placed, out_specs=P("wide", None, "fields"), check_vma=False
    )
```

```python
import jax
import jax.numpy as jnp
from jax import lax
from jax.experimental import pallas as pl
from jax.experimental.pallas import tpu as pltpu
from jax.sharding import PartitionSpec as P


STEPS = 4
UNROLL = 32
LANES = 128
SUBLANES = 8
SHARE_ROWS = SUBLANES + 1


def from_behind(value, axis, steps):
    count = lax.axis_size(axis)
    pairs = [(source, (source + steps) % count) for source in range(count)]
    return lax.ppermute(value, axis, pairs)


def to_everyone(copies, axis, groups=None):
    return lax.all_to_all(
        copies, axis, split_axis=0, concat_axis=0, tiled=True, axis_index_groups=groups
    )


def block_distance(ids_ref, q, row_count, behind, blocks):
    return lax.rem(behind - lax.div(ids_ref[q], row_count) + blocks, blocks)


def spread_kernel(ids_ref, place_ref, *refs):
    held_refs = refs[:STEPS]
    copies_ref, held_ref, rows_ref = refs[STEPS + 1 :]
    row_count = held_refs[0].shape[0]
    blocks = copies_ref.shape[0] * STEPS
    for step, ref in enumerate(held_refs):
        held_ref[step] = ref[...]
    for q in range(rows_ref.shape[0]):
        step = lax.min(block_distance(ids_ref, q, row_count, place_ref[0], blocks), STEPS - 1)
        rows_ref[q : q + 1, :] = held_ref[step, pl.ds(lax.rem(ids_ref[q], row_count), 1), :]
    rows = rows_ref[...]
    for peer in range(copies_ref.shape[0]):
        copies_ref[peer] = rows


def lane_at(offset):
    lane = lax.broadcasted_iota(jnp.int32, (SUBLANES, LANES), 1)
    sublane = lax.broadcasted_iota(jnp.int32, (SUBLANES, LANES), 0)
    return lane == sublane + offset


def column_sum(tiles):
    folded = tiles[0]
    for tile in tiles[1:]:
        folded = folded + tile
    return jnp.sum(folded, axis=1, keepdims=True)


def by_group(columns):
    lane = lax.broadcasted_iota(jnp.int32, (SUBLANES, LANES), 1)
    size = LANES // len(columns)
    tile = jnp.broadcast_to(columns[-1], (SUBLANES, LANES))
    for g in range(len(columns) - 2, -1, -1):
        tile = jnp.where(lane < (g + 1) * size, columns[g], tile)
    return tile


def every_row(ref, row):
    return jnp.broadcast_to(ref[pl.ds(row, 1), :], (SUBLANES, LANES))


def turn_kernel(own_ref, turned_ref):
    row_count, width = own_ref.shape
    for t in range(width // LANES):
        at = slice(t * LANES, (t + 1) * LANES)
        for a in range(SUBLANES):
            rows = jnp.concatenate(
                [
                    jnp.broadcast_to(own_ref[v : v + 1, at], (row_count, LANES))
                    for v in range(a, row_count, SUBLANES)
                ],
                axis=0,
            )
            turned_ref[pl.ds(t * LANES * SUBLANES + a, LANES, stride=SUBLANES), :] = rows.T


def table_kernel(ids_ref, place_ref, own_ref, turned_ref, arrived_ref, *refs):
    partner_refs = refs[:STEPS]
    out_ref, pivots_ref, fields_ref, splat_ref = refs[STEPS:]
    row_count, width = own_ref.shape
    pivot_count = pivots_ref.shape[0]
    tiles = width // LANES
    groups = row_count // SUBLANES
    peers = arrived_ref.shape[0]
    for q in range(pivot_count):
        ahead = lax.div(
            block_distance(ids_ref, q, row_count, place_ref[0], peers * STEPS), STEPS
        )
        peer = lax.rem(lax.div(place_ref[0], STEPS) - ahead + peers, peers)
        pivots_ref[q : q + 1, :] = arrived_ref[peer, q : q + 1, :]

    for t in range(tiles):
        at = slice(t * LANES, (t + 1) * LANES)
        for cg in range(groups):
            rows = [ref[cg * SUBLANES : (cg + 1) * SUBLANES, at] for ref in partner_refs]
            fields_ref[cg * width + t * LANES : cg * width + (t + 1) * LANES, :] = jnp.concatenate(
                rows * groups, axis=0
            ).T
        for q in range(pivot_count):
            splat_ref[q * width + t * LANES : q * width + (t + 1) * LANES, :] = jnp.broadcast_to(
                pivots_ref[q : q + 1, at], (LANES, LANES)
            ).T

    def some_fields(step, sums):
        sums = list(sums)
        for i in range(UNROLL):
            f = step * UNROLL + i
            own = turned_ref[pl.ds(f * SUBLANES, SUBLANES), :]
            partners = [every_row(fields_ref, cg * width + f) for cg in range(groups)]
            for q in range(pivot_count):
                larger = jnp.maximum(own, every_row(splat_ref, q * width + f))
                for cg in range(groups):
                    k = q * groups + cg
                    sums[k] = sums[k] + jnp.minimum(larger, partners[cg])
        return tuple(sums)

    first = []
    for q in range(pivot_count):
        smaller = by_group(
            [
                column_sum(
                    [
                        jnp.minimum(
                            own_ref[g * SUBLANES : (g + 1) * SUBLANES, t * LANES : (t + 1) * LANES],
                            pivots_ref[q : q + 1, t * LANES : (t + 1) * LANES],
                        )
                        for t in range(tiles)
                    ]
                )
                for g in range(groups)
            ]
        )
        first.extend([smaller] * groups)
    sums = lax.fori_loop(0, width // UNROLL, some_fields, tuple(first))

    def totals(ref, g):
        rows = slice(g * SUBLANES, (g + 1) * SUBLANES)
        return column_sum([ref[rows, t * LANES : (t + 1) * LANES] for t in range(tiles)])

    own_row = jnp.zeros((SUBLANES, LANES), jnp.float32)
    for g in range(groups):
        own_row = own_row + jnp.where(lane_at(row_count + g * SUBLANES), totals(own_ref, g), 0.0)
    own_row = jnp.sum(own_row, axis=0, keepdims=True) + totals(pivots_ref, 0)
    lane = lax.broadcasted_iota(jnp.int32, (SUBLANES, LANES), 1)
    for cg in range(groups):
        partner_row = jnp.sum(fields_ref[cg * width : (cg + 1) * width, :], axis=0, keepdims=True)
        rows = jnp.where(lane < STEPS * SUBLANES, partner_row, own_row)
        for q in range(pivot_count):
            at = (q * groups + cg) * SHARE_ROWS
            out_ref[at : at + SUBLANES, :] = sums[q * groups + cg]
            out_ref[at + SUBLANES : at + SUBLANES + 1, :] = rows[q : q + 1, :]


def quotient_kernel(arrived_ref, out_ref):
    steps, _, row_count = out_ref.shape
    peers = arrived_ref.shape[0] // SHARE_ROWS
    groups = row_count // SUBLANES
    size = LANES // groups
    numerator = arrived_ref[0:SUBLANES, :]
    total = arrived_ref[SUBLANES : SUBLANES + 1, :]
    for peer in range(1, peers):
        at = peer * SHARE_ROWS
        numerator = numerator + arrived_ref[at : at + SUBLANES, :]
        total = total + arrived_ref[at + SUBLANES : at + SUBLANES + 1, :]
    totals = jnp.broadcast_to(total, (SUBLANES, LANES))
    own = by_group(
        [
            jnp.sum(jnp.where(lane_at(size + g * SUBLANES), totals, 0.0), axis=1, keepdims=True)
            for g in range(groups)
        ]
    )
    partner = jnp.concatenate([totals[:, :size]] * groups, axis=1)
    turned = (1.5 * numerator / (own + partner)).T
    for s in range(steps):
        rows = [g * size + s * SUBLANES for g in range(groups)]
        out_ref[s] = jnp.concatenate([turned[r : r + SUBLANES, :] for r in rows], axis=1)


def in_vmem(array):
    return pltpu.with_memory_space_constraint(array, pltpu.VMEM)


def body(vectors, pivot_ids):
    row_count, width = vectors.shape
    pivot_count = pivot_ids.shape[0]
    wide = lax.axis_size("wide")
    fields = lax.axis_size("fields")
    smem = pl.BlockSpec(memory_space=pltpu.SMEM)
    vmem = pl.BlockSpec(memory_space=pltpu.VMEM)
    small = pltpu.CompilerParams(vmem_limit_bytes=16 << 20)
    peers = wide // STEPS
    apart = [[first + STEPS * peer for peer in range(peers)] for first in range(STEPS)]
    place = lax.axis_index("wide").astype(jnp.int32).reshape(1)
    partners = []
    for s in range(1, STEPS + 1):
        partners.append(from_behind(vectors, "wide", s))
    turned = pl.pallas_call(
        turn_kernel,
        out_shape=pltpu.VMEM((width * SUBLANES, LANES), jnp.float32),
        in_specs=[vmem],
        out_specs=vmem,
        compiler_params=small,
        name="turn",
    )(in_vmem(vectors))
    copies = pl.pallas_call(
        spread_kernel,
        out_shape=pltpu.VMEM((peers, pivot_count, width), jnp.float32),
        in_specs=[smem] * 2 + [vmem] * (1 + STEPS),
        out_specs=vmem,
        scratch_shapes=[
            pltpu.VMEM((STEPS, row_count, width), jnp.float32),
            pltpu.VMEM((pivot_count, width), jnp.float32),
        ],
        compiler_params=small,
        name="spread",
    )(pivot_ids, place, *(in_vmem(a) for a in (vectors, *partners)))
    arrived = to_everyone(copies, "wide", apart)
    table = pl.pallas_call(
        table_kernel,
        out_shape=pltpu.VMEM((fields * SHARE_ROWS, LANES), jnp.float32),
        in_specs=[smem] * 2 + [vmem] * (3 + STEPS),
        out_specs=vmem,
        scratch_shapes=[
            pltpu.VMEM((pivot_count, width), jnp.float32),
            pltpu.VMEM((row_count // SUBLANES * width, LANES), jnp.float32),
            pltpu.VMEM((pivot_count * width, LANES), jnp.float32),
        ],
        compiler_params=small,
        name="table",
    )(pivot_ids, place, *(in_vmem(a) for a in (vectors, turned, arrived, *partners)))
    shares = to_everyone(table.reshape(fields, 1, SHARE_ROWS * LANES), "fields")
    quotient = pl.pallas_call(
        quotient_kernel,
        out_shape=jax.ShapeDtypeStruct((STEPS, SUBLANES, row_count), jnp.float32),
        in_specs=[vmem],
        out_specs=vmem,
        name="quotient",
    )(in_vmem(shares.reshape(fields * SHARE_ROWS, LANES)))
    return jnp.transpose(quotient, (2, 0, 1))


def solution(mesh):
    placed = (P("wide", "fields"), P())
    return jax.shard_map(
        body, mesh=mesh, in_specs=placed, out_specs=P("wide", None, "fields"), check_vma=False
    )
```

```python
import jax
import jax.numpy as jnp
from jax import lax
from jax.experimental import pallas as pl
from jax.experimental.pallas import tpu as pltpu
from jax.sharding import PartitionSpec as P


STEPS = 4
UNROLL = 32
LANES = 128
SUBLANES = 8
SHARE_ROWS = SUBLANES + 1


def from_behind(value, axis, steps):
    count = lax.axis_size(axis)
    pairs = [(source, (source + steps) % count) for source in range(count)]
    return lax.ppermute(value, axis, pairs)


def to_everyone(copies, axis, groups=None):
    return lax.all_to_all(
        copies, axis, split_axis=0, concat_axis=0, tiled=True, axis_index_groups=groups
    )


def block_distance(ids_ref, q, row_count, behind, blocks):
    return lax.rem(behind - lax.div(ids_ref[q], row_count) + blocks, blocks)


def spread_kernel(ids_ref, place_ref, *refs):
    held_refs = refs[:STEPS]
    copies_ref, held_ref, rows_ref = refs[STEPS:]
    row_count = held_refs[0].shape[0]
    blocks = copies_ref.shape[0] * STEPS
    for step, ref in enumerate(held_refs):
        held_ref[step] = ref[...]
    for q in range(rows_ref.shape[0]):
        step = lax.min(block_distance(ids_ref, q, row_count, place_ref[0], blocks), STEPS - 1)
        rows_ref[q : q + 1, :] = held_ref[step, pl.ds(lax.rem(ids_ref[q], row_count), 1), :]
    rows = rows_ref[...]
    for peer in range(copies_ref.shape[0]):
        copies_ref[peer] = rows


def lane_at(offset):
    lane = lax.broadcasted_iota(jnp.int32, (SUBLANES, LANES), 1)
    sublane = lax.broadcasted_iota(jnp.int32, (SUBLANES, LANES), 0)
    return lane == sublane + offset


def column_sum(tiles):
    folded = tiles[0]
    for tile in tiles[1:]:
        folded = folded + tile
    return jnp.sum(folded, axis=1, keepdims=True)


def by_group(columns):
    lane = lax.broadcasted_iota(jnp.int32, (SUBLANES, LANES), 1)
    size = LANES // len(columns)
    tile = jnp.broadcast_to(columns[-1], (SUBLANES, LANES))
    for g in range(len(columns) - 2, -1, -1):
        tile = jnp.where(lane < (g + 1) * size, columns[g], tile)
    return tile


def every_row(ref, row):
    return jnp.broadcast_to(ref[pl.ds(row, 1), :], (SUBLANES, LANES))


def turn_kernel(own_ref, turned_ref):
    row_count, width = own_ref.shape
    for t in range(width // LANES):
        at = slice(t * LANES, (t + 1) * LANES)
        for a in range(SUBLANES):
            rows = jnp.concatenate(
                [
                    jnp.broadcast_to(own_ref[v : v + 1, at], (row_count, LANES))
                    for v in range(a, row_count, SUBLANES)
                ],
                axis=0,
            )
            turned_ref[pl.ds(t * LANES * SUBLANES + a, LANES, stride=SUBLANES), :] = rows.T


def partners_kernel(*refs):
    partner_refs = refs[:STEPS]
    (fields_ref,) = refs[STEPS:]
    row_count, width = partner_refs[0].shape
    groups = row_count // SUBLANES
    for t in range(width // LANES):
        at = slice(t * LANES, (t + 1) * LANES)
        for cg in range(groups):
            rows = [ref[cg * SUBLANES : (cg + 1) * SUBLANES, at] for ref in partner_refs]
            fields_ref[cg * width + t * LANES : cg * width + (t + 1) * LANES, :] = jnp.concatenate(
                rows * groups, axis=0
            ).T


def table_kernel(
    ids_ref, place_ref, own_ref, turned_ref, fields_ref, arrived_ref, out_ref, pivots_ref, splat_ref
):
    row_count, width = own_ref.shape
    pivot_count = pivots_ref.shape[0]
    tiles = width // LANES
    groups = row_count // SUBLANES
    peers = arrived_ref.shape[0]
    for q in range(pivot_count):
        ahead = lax.div(
            block_distance(ids_ref, q, row_count, place_ref[0], peers * STEPS), STEPS
        )
        peer = lax.rem(lax.div(place_ref[0], STEPS) - ahead + peers, peers)
        pivots_ref[q : q + 1, :] = arrived_ref[peer, q : q + 1, :]

    pivots = pivots_ref[...]
    high = pivots.astype(jnp.bfloat16).astype(jnp.float32)
    rest = pivots - high
    middle = rest.astype(jnp.bfloat16).astype(jnp.float32)
    parts = jnp.concatenate([high, middle, rest - middle, jnp.zeros_like(high)], axis=0)
    parts = parts.astype(jnp.bfloat16)
    shape = (parts.shape[0], pivot_count * LANES)
    part = lax.broadcasted_iota(jnp.int32, shape, 0)
    lane = lax.broadcasted_iota(jnp.int32, shape, 1)
    chosen = jnp.where(lax.rem(part, pivot_count) == lax.div(lane, LANES), 1.0, 0.0)
    chosen = chosen.astype(jnp.bfloat16)
    for t in range(tiles):
        splat = lax.dot_general(
            parts[:, t * LANES : (t + 1) * LANES],
            chosen,
            (((0,), (0,)), ((), ())),
            preferred_element_type=jnp.float32,
        )
        for q in range(pivot_count):
            splat_ref[q * width + t * LANES : q * width + (t + 1) * LANES, :] = splat[
                :, q * LANES : (q + 1) * LANES
            ]

    def some_fields(step, sums):
        sums = list(sums)
        for i in range(UNROLL):
            f = step * UNROLL + i
            own = turned_ref[pl.ds(f * SUBLANES, SUBLANES), :]
            partners = [every_row(fields_ref, cg * width + f) for cg in range(groups)]
            for q in range(pivot_count):
                larger = jnp.maximum(own, every_row(splat_ref, q * width + f))
                for cg in range(groups):
                    k = q * groups + cg
                    sums[k] = sums[k] + jnp.minimum(larger, partners[cg])
        return tuple(sums)

    first = []
    for q in range(pivot_count):
        smaller = by_group(
            [
                column_sum(
                    [
                        jnp.minimum(
                            own_ref[g * SUBLANES : (g + 1) * SUBLANES, t * LANES : (t + 1) * LANES],
                            pivots_ref[q : q + 1, t * LANES : (t + 1) * LANES],
                        )
                        for t in range(tiles)
                    ]
                )
                for g in range(groups)
            ]
        )
        first.extend([smaller] * groups)
    sums = lax.fori_loop(0, width // UNROLL, some_fields, tuple(first))

    def totals(ref, g):
        rows = slice(g * SUBLANES, (g + 1) * SUBLANES)
        return column_sum([ref[rows, t * LANES : (t + 1) * LANES] for t in range(tiles)])

    own_row = jnp.zeros((SUBLANES, LANES), jnp.float32)
    for g in range(groups):
        own_row = own_row + jnp.where(lane_at(row_count + g * SUBLANES), totals(own_ref, g), 0.0)
    own_row = jnp.sum(own_row, axis=0, keepdims=True) + totals(pivots_ref, 0)
    lane = lax.broadcasted_iota(jnp.int32, (SUBLANES, LANES), 1)
    for cg in range(groups):
        partner_row = jnp.sum(fields_ref[cg * width : (cg + 1) * width, :], axis=0, keepdims=True)
        rows = jnp.where(lane < STEPS * SUBLANES, partner_row, own_row)
        for q in range(pivot_count):
            at = (q * groups + cg) * SHARE_ROWS
            out_ref[at : at + SUBLANES, :] = sums[q * groups + cg]
            out_ref[at + SUBLANES : at + SUBLANES + 1, :] = rows[q : q + 1, :]


def quotient_kernel(arrived_ref, out_ref):
    steps, _, row_count = out_ref.shape
    peers = arrived_ref.shape[0] // SHARE_ROWS
    groups = row_count // SUBLANES
    size = LANES // groups
    numerator = arrived_ref[0:SUBLANES, :]
    total = arrived_ref[SUBLANES : SUBLANES + 1, :]
    for peer in range(1, peers):
        at = peer * SHARE_ROWS
        numerator = numerator + arrived_ref[at : at + SUBLANES, :]
        total = total + arrived_ref[at + SUBLANES : at + SUBLANES + 1, :]
    totals = jnp.broadcast_to(total, (SUBLANES, LANES))
    own = by_group(
        [
            jnp.sum(jnp.where(lane_at(size + g * SUBLANES), totals, 0.0), axis=1, keepdims=True)
            for g in range(groups)
        ]
    )
    partner = jnp.concatenate([totals[:, :size]] * groups, axis=1)
    turned = (1.5 * numerator / (own + partner)).T
    for s in range(steps):
        rows = [g * size + s * SUBLANES for g in range(groups)]
        out_ref[s] = jnp.concatenate([turned[r : r + SUBLANES, :] for r in rows], axis=1)


def in_vmem(array):
    return pltpu.with_memory_space_constraint(array, pltpu.VMEM)


def body(vectors, pivot_ids):
    row_count, width = vectors.shape
    pivot_count = pivot_ids.shape[0]
    wide = lax.axis_size("wide")
    fields = lax.axis_size("fields")
    smem = pl.BlockSpec(memory_space=pltpu.SMEM)
    vmem = pl.BlockSpec(memory_space=pltpu.VMEM)
    small = pltpu.CompilerParams(vmem_limit_bytes=16 << 20)
    peers = wide // STEPS
    apart = [[first + STEPS * peer for peer in range(peers)] for first in range(STEPS)]
    place = lax.axis_index("wide").astype(jnp.int32).reshape(1)
    partners = []
    for s in range(1, STEPS + 1):
        partners.append(from_behind(vectors, "wide", s))
    turned = pl.pallas_call(
        turn_kernel,
        out_shape=pltpu.VMEM((width * SUBLANES, LANES), jnp.float32),
        in_specs=[vmem],
        out_specs=vmem,
        compiler_params=small,
        name="turn",
    )(in_vmem(vectors))
    copies = pl.pallas_call(
        spread_kernel,
        out_shape=jax.ShapeDtypeStruct((peers, pivot_count, width), jnp.float32),
        in_specs=[smem] * 2 + [vmem] * STEPS,
        out_specs=vmem,
        scratch_shapes=[
            pltpu.VMEM((STEPS, row_count, width), jnp.float32),
            pltpu.VMEM((pivot_count, width), jnp.float32),
        ],
        compiler_params=small,
        name="spread",
    )(pivot_ids, place, *(in_vmem(a) for a in (vectors, *partners[:-1])))
    arrived = to_everyone(copies, "wide", apart)
    turned_partners = pl.pallas_call(
        partners_kernel,
        out_shape=pltpu.VMEM((row_count // SUBLANES * width, LANES), jnp.float32),
        in_specs=[vmem] * STEPS,
        out_specs=vmem,
        compiler_params=small,
        name="partners",
    )(*(in_vmem(a) for a in partners))
    table = pl.pallas_call(
        table_kernel,
        out_shape=pltpu.VMEM((fields * SHARE_ROWS, LANES), jnp.float32),
        in_specs=[smem] * 2 + [vmem] * 4,
        out_specs=vmem,
        scratch_shapes=[
            pltpu.VMEM((pivot_count, width), jnp.float32),
            pltpu.VMEM((pivot_count * width, LANES), jnp.float32),
        ],
        compiler_params=small,
        name="table",
    )(pivot_ids, place, *(in_vmem(a) for a in (vectors, turned, turned_partners, arrived)))
    shares = to_everyone(table.reshape(fields, 1, SHARE_ROWS * LANES), "fields")
    quotient = pl.pallas_call(
        quotient_kernel,
        out_shape=jax.ShapeDtypeStruct((STEPS, SUBLANES, row_count), jnp.float32),
        in_specs=[vmem],
        out_specs=vmem,
        name="quotient",
    )(in_vmem(shares.reshape(fields * SHARE_ROWS, LANES)))
    return jnp.transpose(quotient, (2, 0, 1))


def solution(mesh):
    placed = (P("wide", "fields"), P())
    return jax.shard_map(
        body, mesh=mesh, in_specs=placed, out_specs=P("wide", None, "fields"), check_vma=False
    )
```
